32 devices in a mesh: space: 16 (over z, y, x), tm: 2 (over core).
Axes of the slice: x: 2, y: 2, z: 4, core: 2. Of those that a mesh axis runs over, the one named last changes fastest.
Arguments:
- vectors: bfloat16 [2, 64, 2, 12, 2048], P('tm', None, None, None, 'space'), may hold values from -6 to 6
- dilution: int32 [64], replicated, may hold values from 0 to 23
- gamma_ids: int32 [16], replicated, may hold values from 1 to 15
Outputs:
- gram: float32 [2, 1024, 128], P(None, 'space')
- loops: float32 [2, 1024, 2], P(None, 'space')
The draws below stay inside these ranges and needn't reach their ends.
All inputs are finite; a program needn't handle non-finite values.
Results may differ from the reference program's by a relative error of at most 0.0003.
Values sent between devices are 32-bit elements; how exact they have to be, the bound alone decides.
A program may use at most 64 MiB of HBM per device.

```python
import math
from functools import partial
import jax
import jax.numpy as jnp
from jax import lax

NVEC = 64
NG = 16
TDIL = 2
NSITES = 2048
NT = 2


def touch_ends(result, rng, least, largest):
    shape = result.shape
    place = [jax.random.randint(jax.random.fold_in(rng, axis), (), 0, shape[axis]) for axis in range(len(shape))]
    result = result.at[tuple(place)].set(least)
    longest = shape.index(max(shape))
    place[longest] = (place[longest] + 1) % shape[longest]
    return result.at[tuple(place)].set(largest)


def level_of(own_key, extent, shards, smallest, largest):
    def one(dim, parts):
        steps = jax.random.uniform(jax.random.fold_in(jax.random.fold_in(own_key, 6), dim), (parts,), jnp.float32, smallest / len(shards), largest / len(shards))
        return jnp.repeat(jnp.exp(steps), extent[dim] // parts).reshape((-1,) + (1,) * (len(extent) - dim - 1))

    factor_of = one(*shards[0])
    for cut in shards[1:]:
        factor_of = factor_of * one(*cut)
    return factor_of


def noise(rng, dims, spread, bound, pieces=(), held_as=jnp.bfloat16):
    result = spread * jax.random.normal(rng, dims, jnp.float32)
    if pieces:
        result = result * level_of(rng, dims, pieces, -0.22, 0.18)
    return jnp.clip(result, -bound, bound).astype(held_as)


def setup_inputs(seed: int = 0) -> dict:
    arg_keys = jax.random.split(jax.random.key(seed), 4)
    return {
        "vectors": noise(arg_keys[0], (NT, NVEC, 2, 12, NSITES), 1.0, 6.0, ((0, 2), (4, 16))),
        "dilution": touch_ends(jax.random.randint(arg_keys[1], (NVEC,), 0, 12 * TDIL), jax.random.fold_in(arg_keys[1], 1), 0, (12 * TDIL) - 1).astype(jnp.int32),
        "gamma_ids": touch_ends(jax.random.randint(arg_keys[2], (NG,), 1, 16), jax.random.fold_in(arg_keys[2], 1), 1, 15).astype(jnp.int32),
    }


highest = lax.Precision.HIGHEST

def zero_square():
    return [[0, 0, 0, 0] for _ in range(4)]

def pair_product(left, right):
    real_out = zero_square()
    imag_out = zero_square()
    for row in range(4):
        for col in range(4):
            acc_real = 0
            acc_imag = 0
            for mid in range(4):
                acc_real += left[0][row][mid] * right[0][mid][col] - left[1][row][mid] * right[1][mid][col]
                acc_imag += left[0][row][mid] * right[1][mid][col] + left[1][row][mid] * right[0][mid][col]
            real_out[row][col] = acc_real
            imag_out[row][col] = acc_imag
    return (real_out, imag_out)

def dirac_tables():
    factors = [(zero_square(), [[0, 0, 0, 1], [0, 0, 1, 0], [0, -1, 0, 0], [-1, 0, 0, 0]]), ([[0, 0, 0, -1], [0, 0, 1, 0], [0, 1, 0, 0], [-1, 0, 0, 0]], zero_square()), (zero_square(), [[0, 0, 1, 0], [0, 0, 0, -1], [-1, 0, 0, 0], [0, 1, 0, 0]]), ([[0, 0, 1, 0], [0, 0, 0, 1], [1, 0, 0, 0], [0, 1, 0, 0]], zero_square())]
    reals = []
    imags = []
    for number in range(16):
        current = ([[1 if a == b else 0 for b in range(4)] for a in range(4)], zero_square())
        for position in range(4):
            if number >> position & 1:
                current = pair_product(current, factors[position])
        reals.append([value for line in current[0] for value in line])
        imags.append([value for line in current[1] for value in line])
    return (reals, imags)

def pick_gammas(gamma_ids):
    table_real, table_imag = dirac_tables()
    choose = (gamma_ids[:, None] == jnp.arange(16, dtype=jnp.int32)[None, :]).astype(jnp.float32)
    gamma_real = jnp.dot(choose, jnp.asarray(table_real, dtype=jnp.float32), precision=highest).reshape(-1, 4, 4)
    gamma_imag = jnp.dot(choose, jnp.asarray(table_imag, dtype=jnp.float32), precision=highest).reshape(-1, 4, 4)
    return (gamma_real, gamma_imag)

def reference(vectors, dilution, gamma_ids):
    times, count, halves, comps, sites = vectors.shape
    gamma_real, gamma_imag = pick_gammas(gamma_ids)
    gram_scale = 1.0 / math.sqrt(48.0 * sites)
    loop_scale = 1.0 / math.sqrt(1.0 * sites)
    spin_pick = ((dilution % 12 // 3)[:, None] == jnp.arange(4, dtype=jnp.int32)[None, :]).astype(jnp.float32)
    colour_pick = ((dilution % 3)[:, None] == jnp.arange(3, dtype=jnp.int32)[None, :]).astype(jnp.float32)
    time_class = dilution // 12
    ein = partial(jnp.einsum, precision=highest)

    def one_slice(inputs):
        block, slice_index = inputs
        field = block.astype(jnp.float32).reshape(count, 2, 4, 3, sites)
        real_part = field[:, 0]
        imag_part = field[:, 1]
        pair_real = ein('iack,jbck->iajb', real_part, real_part) + ein('iack,jbck->iajb', imag_part, imag_part)
        pair_imag = ein('iack,jbck->iajb', real_part, imag_part) - ein('iack,jbck->iajb', imag_part, real_part)
        gram_real = ein('gab,iajb->gij', gamma_real, pair_real) - ein('gab,iajb->gij', gamma_imag, pair_imag)
        gram_imag = ein('gab,iajb->gij', gamma_real, pair_imag) + ein('gab,iajb->gij', gamma_imag, pair_real)
        gram = jnp.concatenate([gram_real, gram_imag], axis=2).reshape(-1, 2 * count) * gram_scale
        site_sums = lax.optimization_barrier(jnp.sum(field, axis=-1))
        picked = ein('ipac,ic->ipa', site_sums, colour_pick)
        rows_real = ein('gba,ib->gia', gamma_real, spin_pick)
        rows_imag = ein('gba,ib->gia', gamma_imag, spin_pick)
        loop_real = ein('gia,ia->gi', rows_real, picked[:, 0]) - ein('gia,ia->gi', rows_imag, picked[:, 1])
        loop_imag = ein('gia,ia->gi', rows_real, picked[:, 1]) + ein('gia,ia->gi', rows_imag, picked[:, 0])
        live = (time_class == slice_index % TDIL).astype(jnp.float32)[None, :]
        loops = jnp.stack([loop_real * live, loop_imag * live], axis=-1).reshape(-1, 2) * loop_scale
        return (gram, loops)
    gram, loops = lax.map(one_slice, (vectors, jnp.arange(times, dtype=jnp.int32)))
    return (gram, loops)
```

```python
from functools import partial
import math

import jax
import jax.numpy as jnp
from jax import lax
from jax.experimental import pallas as pl
from jax.experimental.pallas import tpu as pltpu
from jax.sharding import PartitionSpec as P

TDIL = 2


highest = lax.Precision.HIGHEST


def zero_square():
    return [[0, 0, 0, 0] for _ in range(4)]


def pair_product(left, right):
    real_out = zero_square()
    imag_out = zero_square()
    for row in range(4):
        for col in range(4):
            acc_real = 0
            acc_imag = 0
            for mid in range(4):
                acc_real += (
                    left[0][row][mid] * right[0][mid][col] - left[1][row][mid] * right[1][mid][col]
                )
                acc_imag += (
                    left[0][row][mid] * right[1][mid][col] + left[1][row][mid] * right[0][mid][col]
                )
            real_out[row][col] = acc_real
            imag_out[row][col] = acc_imag
    return (real_out, imag_out)


def dirac_tables():
    factors = [
        (zero_square(), [[0, 0, 0, 1], [0, 0, 1, 0], [0, -1, 0, 0], [-1, 0, 0, 0]]),
        ([[0, 0, 0, -1], [0, 0, 1, 0], [0, 1, 0, 0], [-1, 0, 0, 0]], zero_square()),
        (zero_square(), [[0, 0, 1, 0], [0, 0, 0, -1], [-1, 0, 0, 0], [0, 1, 0, 0]]),
        ([[0, 0, 1, 0], [0, 0, 0, 1], [1, 0, 0, 0], [0, 1, 0, 0]], zero_square()),
    ]
    reals = []
    imags = []
    for number in range(16):
        current = ([[1 if a == b else 0 for b in range(4)] for a in range(4)], zero_square())
        for position in range(4):
            if number >> position & 1:
                current = pair_product(current, factors[position])
        reals.append([value for line in current[0] for value in line])
        imags.append([value for line in current[1] for value in line])
    return (reals, imags)


def pick_gammas(gamma_ids):
    table_real, table_imag = dirac_tables()
    choose = (gamma_ids[:, None] == jnp.arange(16, dtype=jnp.int32)[None, :]).astype(jnp.float32)
    gamma_real = jnp.dot(
        choose, jnp.asarray(table_real, dtype=jnp.float32), precision=highest
    ).reshape(-1, 4, 4)
    gamma_imag = jnp.dot(
        choose, jnp.asarray(table_imag, dtype=jnp.float32), precision=highest
    ).reshape(-1, 4, 4)
    return (gamma_real, gamma_imag)


MESH = pl.DeviceIdType.MESH
SPINS = 4
COLOURS = 3
COMPS = SPINS * COLOURS
LANES = 128


def gamma_entries():
    reals, imags = dirac_tables()
    out = []
    for re, im in zip(reals, imags):
        rows = []
        for a in range(SPINS):
            (b,) = [b for b in range(SPINS) if re[a * SPINS + b] or im[a * SPINS + b]]
            rows.append((b, re[a * SPINS + b], im[a * SPINS + b]))
        anti = any(
            (rows[b][1], rows[b][2]) != (re_ab, -im_ab) for b, re_ab, im_ab in rows
        )
        out.append((anti, rows))
    return out


def kernel(
    owners, groups, per_owner, gram_scale, loop_scale,
    ids_ref, dil_ref, vec_ref, gram_ref, loops_ref,
    raw, wide, stack, pairs, packed, sendbuf, recvbuf, mine, theirs,
    load_sem, send_sem, recv_sem, swap_send, swap_recv,
):
    count = vec_ref.shape[0]
    half = count // 2
    space = lax.axis_index("space")
    time = lax.axis_index("tm")
    load = pltpu.make_async_copy(vec_ref, raw, load_sem)
    load.start()
    barrier = pltpu.get_barrier_semaphore()
    for step in range(1, owners):
        pl.semaphore_signal(
            barrier, inc=1, device_id=(lax.rem(space + step, owners), time), device_id_type=MESH
        )
    for step in range(1, groups):
        pl.semaphore_signal(
            barrier, inc=1, device_id=(space, lax.rem(time + step, groups)), device_id_type=MESH
        )
    load.wait()

    for i in range(count):
        for p in range(2):
            at = (2 * i + p) * COMPS
            wide[at : at + COMPS, :] = raw[i, p].astype(jnp.float32)
    for a in range(SPINS):
        for p in range(2):
            for c in range(COLOURS):
                rows = wide[pl.ds(p * COMPS + COLOURS * a + c, count, stride=2 * COMPS), :]
                at = (2 * a + p) * count
                stack[at : at + count, c * LANES : (c + 1) * LANES] = rows.astype(jnp.bfloat16)
    everything = stack[...]
    contract = (((1,), (1,)), ((), ()))
    pairs[...] = lax.dot_general(
        everything, everything, contract, preferred_element_type=jnp.float32
    )

    lane = lax.broadcasted_iota(jnp.int32, (1, 2 * count), 1)
    left = lane < count
    turn = jnp.where(left, -1.0, 1.0).astype(jnp.float32)
    dil = dil_ref[...]
    dil = jnp.concatenate([dil, dil], axis=1)
    comp = lax.rem(dil, COMPS)
    spin = lax.div(comp, COLOURS)
    colour = lax.rem(comp, COLOURS)
    live = lax.div(dil, COMPS) == lax.rem(time, TDIL)
    ones = jnp.ones((8, LANES), jnp.bfloat16)
    sums = [
        lax.dot_general(
            ones, everything[:, c * LANES : (c + 1) * LANES], contract,
            preferred_element_type=jnp.float32,
        )
        for c in range(COLOURS)
    ]
    quark = []
    for a in range(SPINS):
        got = sums[COLOURS - 1][:, a * LANES : (a + 1) * LANES]
        for c in range(COLOURS - 1):
            got = jnp.where(colour == c, sums[c][:, a * LANES : (a + 1) * LANES], got)
        got = jnp.where(live, got, 0.0)
        quark.append((got, pltpu.roll(got, count, 1) * turn))

    row = lax.broadcasted_iota(jnp.int32, (half, 2 * count), 0)
    col = lax.broadcasted_iota(jnp.int32, (half, 2 * count), 1)
    upper = row <= col
    lower = row + half > col - count
    low_lanes = col < count

    def block(a, b):
        first = pairs[2 * a * count : (2 * a + 1) * count, b * LANES : (b + 1) * LANES]
        second = pairs[(2 * a + 1) * count : (2 * a + 2) * count, b * LANES : (b + 1) * LANES]
        return first - turn * pltpu.roll(second, count, 1)

    entries = gamma_entries()
    for shift in range(SPINS):
        plain = [block(a, a ^ shift) for a in range(SPINS)]
        turned = [pltpu.roll(x, count, 1) * turn for x in plain]
        for number, (anti, rows) in enumerate(entries):
            if rows[0][0] != shift or number == 0:
                continue
            total = None
            loop = jnp.zeros_like(quark[0][0])
            for a, (b, re, im) in enumerate(rows):
                term = quark[b][0] if re else quark[b][1]
                loop = jnp.where(spin == a, term if re + im > 0 else -term, loop)
                if anti:
                    re, im = im, -re
                term = plain[a] if re else turned[a]
                if total is None:
                    total = term if re + im > 0 else -term
                else:
                    total = total + term if re + im > 0 else total - term
            top, bottom = total[:half], total[half:]
            top = jnp.where(upper, top, pltpu.roll(top, count, 1))
            bottom = jnp.where(lower, bottom, pltpu.roll(bottom, count, 1))
            packed[number, 0:half, :] = jnp.where(low_lanes, top, bottom)
            packed[number, half : half + 1, :] = loop[0:1]
    for g in range(owners * per_owner):
        sendbuf[g] = packed[ids_ref[g]]

    pl.semaphore_wait(barrier, owners + groups - 2)
    copies = []
    for step in range(1, owners):
        target = lax.rem(space + step, owners)
        copy = pltpu.make_async_remote_copy(
            src_ref=sendbuf.at[pl.ds(target * per_owner, per_owner)],
            dst_ref=recvbuf.at[step - 1],
            send_sem=send_sem.at[step - 1],
            recv_sem=recv_sem.at[step - 1],
            device_id=(target, time),
            device_id_type=MESH,
        )
        copy.start()
        copies.append(copy)
    total = sendbuf[pl.ds(space * per_owner, per_owner)]
    for step in range(1, owners):
        copies[step - 1].wait_recv()
        total = total + recvbuf[step - 1]
    mine[...] = total
    swaps = []
    for step in range(1, groups):
        swap = pltpu.make_async_remote_copy(
            src_ref=mine,
            dst_ref=theirs.at[step - 1],
            send_sem=swap_send.at[step - 1],
            recv_sem=swap_recv.at[step - 1],
            device_id=(space, lax.rem(time + step, groups)),
            device_id_type=MESH,
        )
        swap.start()
        swaps.append(swap)

    above = lax.broadcasted_iota(jnp.int32, (count, 2 * count), 0)
    across = lax.broadcasted_iota(jnp.int32, (count, 2 * count), 1)
    in_real = across < count
    across = jnp.where(in_real, across, across - count)

    def unpack(summed, when):
        for k in range(per_owner):
            part = summed[k, 0:half]
            swapped = pltpu.roll(part, count, 1)
            full = jnp.concatenate(
                [jnp.where(low_lanes, part, swapped), jnp.where(low_lanes, swapped, part)], axis=0
            )
            flipped = jnp.concatenate([full, full], axis=0).T[:count]
            real = jnp.where(above <= across, full, flipped)
            imag = jnp.where(above > across, full, jnp.where(above < across, -flipped, 0.0))
            held = jnp.where(in_real, real, imag)
            number = ids_ref[space * per_owner + k]
            anti = jnp.bool_(False)
            for n, (is_anti, _) in enumerate(entries):
                if is_anti:
                    anti = anti | (number == n)
            rotated = pltpu.roll(held, count, 1) * turn
            out = jnp.where(anti, rotated, held)
            gram_ref[when, k * count : (k + 1) * count, :] = out * gram_scale
            loops_ref[when, k : k + 1, :] = summed[k, half : half + 1] * loop_scale

    unpack(total, time)
    for step in range(1, groups):
        swaps[step - 1].wait_recv()
        unpack(theirs[step - 1], lax.rem(time + groups - step, groups))
    for copy in copies + swaps:
        copy.wait_send()


def packed_shards(vectors, dilution, gamma_ids):
    slices, count, halves, comps, sites = vectors.shape
    owners, groups = lax.axis_size("space"), lax.axis_size("tm")
    numbers = gamma_ids.shape[0]
    per_owner = numbers // owners
    total_sites = sites * owners
    message = (per_owner, count // 2 + 1, 2 * count)
    gram, loops = pl.pallas_call(
        partial(
            kernel, owners, groups, per_owner,
            1.0 / math.sqrt(48.0 * total_sites), 1.0 / math.sqrt(1.0 * total_sites),
        ),
        out_shape=(
            jax.ShapeDtypeStruct((groups, per_owner * count, 2 * count), jnp.float32),
            jax.ShapeDtypeStruct((groups, per_owner, 2 * count), jnp.float32),
        ),
        in_specs=[
            pl.BlockSpec(memory_space=pltpu.SMEM),
            pl.BlockSpec(memory_space=pltpu.VMEM),
            pl.BlockSpec(memory_space=pl.ANY),
        ],
        out_specs=(
            pl.BlockSpec(memory_space=pltpu.VMEM),
            pl.BlockSpec(memory_space=pltpu.VMEM),
        ),
        scratch_shapes=[
            pltpu.VMEM((count, halves, comps, sites), jnp.bfloat16),
            pltpu.VMEM((count * halves * comps, sites), jnp.float32),
            pltpu.VMEM((SPINS * 2 * count, COLOURS * sites), jnp.bfloat16),
            pltpu.VMEM((SPINS * 2 * count, SPINS * 2 * count), jnp.float32),
            pltpu.VMEM((16,) + message[1:], jnp.float32),
            pltpu.VMEM((numbers,) + message[1:], jnp.float32),
            pltpu.VMEM((owners - 1,) + message, jnp.float32),
            pltpu.VMEM(message, jnp.float32),
            pltpu.VMEM((groups - 1,) + message, jnp.float32),
            pltpu.SemaphoreType.DMA,
            pltpu.SemaphoreType.DMA((owners - 1,)),
            pltpu.SemaphoreType.DMA((owners - 1,)),
            pltpu.SemaphoreType.DMA((groups - 1,)),
            pltpu.SemaphoreType.DMA((groups - 1,)),
        ],
        compiler_params=pltpu.CompilerParams(collective_id=0, has_side_effects=True),
    )(gamma_ids, dilution.reshape(1, count), vectors.reshape(count, halves, comps, sites))
    loops = loops.reshape(groups, per_owner, 2, count).swapaxes(2, 3)
    return gram, loops.reshape(groups, per_owner * count, 2)


def any_shards(vectors, dilution, gamma_ids):
    slices, count, halves, comps, sites = vectors.shape
    numbers = gamma_ids.shape[0]
    whole_blocks = numbers % lax.axis_size("space") == 0
    if slices == 1 and sites == LANES and 2 * count == LANES and whole_blocks:
        return packed_shards(vectors, dilution, gamma_ids)
    return shards(vectors, dilution, gamma_ids)


def shards(vectors, dilution, gamma_ids):
    slices, count, halves, comps, sites = vectors.shape
    owners = lax.axis_size("space")
    total_sites = sites * owners
    gram_scale = 1.0 / math.sqrt(48.0 * total_sites)
    loop_scale = 1.0 / math.sqrt(1.0 * total_sites)
    gamma_real, gamma_imag = pick_gammas(gamma_ids)
    spin_pick = ((dilution % 12 // 3)[:, None] == jnp.arange(4, dtype=jnp.int32)[None, :]).astype(
        jnp.float32
    )
    colour_pick = ((dilution % 3)[:, None] == jnp.arange(3, dtype=jnp.int32)[None, :]).astype(
        jnp.float32
    )
    time_class = dilution // 12
    ein = partial(jnp.einsum, precision=highest)
    lowein = partial(jnp.einsum, preferred_element_type=jnp.float32)
    first_slice = lax.axis_index("tm") * slices
    rows_real = ein("gba,ib->gia", gamma_real, spin_pick)
    rows_imag = ein("gba,ib->gia", gamma_imag, spin_pick)

    def one_slice(inputs):
        block, slice_index = inputs
        spinor = block.reshape(count, 2, 4, 3 * sites)
        real_part = spinor[:, 0]
        imag_part = spinor[:, 1]
        pair_real = lowein("iak,jbk->iajb", real_part, real_part) + lowein(
            "iak,jbk->iajb", imag_part, imag_part
        )
        pair_imag = lowein("iak,jbk->iajb", real_part, imag_part) - lowein(
            "iak,jbk->iajb", imag_part, real_part
        )
        gram_real = ein("gab,iajb->gij", gamma_real, pair_real) - ein(
            "gab,iajb->gij", gamma_imag, pair_imag
        )
        gram_imag = ein("gab,iajb->gij", gamma_real, pair_imag) + ein(
            "gab,iajb->gij", gamma_imag, pair_real
        )
        gram = jnp.concatenate([gram_real, gram_imag], axis=2).reshape(-1, 2 * count)
        gram = gram * gram_scale
        site_sums = jnp.sum(block, axis=-1, dtype=jnp.float32).reshape(count, 2, 4, 3)
        picked = ein("ipac,ic->ipa", site_sums, colour_pick)
        loop_real = ein("gia,ia->gi", rows_real, picked[:, 0]) - ein(
            "gia,ia->gi", rows_imag, picked[:, 1]
        )
        loop_imag = ein("gia,ia->gi", rows_real, picked[:, 1]) + ein(
            "gia,ia->gi", rows_imag, picked[:, 0]
        )
        live = (time_class == slice_index % TDIL).astype(jnp.float32)[None, :]
        loops = jnp.stack([loop_real * live, loop_imag * live], axis=-1).reshape(-1, 2) * loop_scale
        return (gram, loops)

    gram_terms, loop_terms = lax.map(
        one_slice, (vectors, first_slice + jnp.arange(slices, dtype=jnp.int32))
    )
    total_rows = gram_terms.shape[1]
    owned = total_rows // owners
    totals = lax.psum((gram_terms, loop_terms), "space")
    start = lax.axis_index("space") * owned
    shares = (
        lax.dynamic_slice_in_dim(totals[0], start, owned, 1),
        lax.dynamic_slice_in_dim(totals[1], start, owned, 1),
    )
    gram, loops = (
        lax.all_gather(shares[0], "tm", axis=0, tiled=True),
        lax.all_gather(shares[1], "tm", axis=0, tiled=True),
    )
    return (gram, loops)


def solution(mesh):
    placed = (P("tm", None, None, None, "space"), P(), P())
    return jax.shard_map(
        any_shards,
        mesh=mesh,
        in_specs=placed,
        out_specs=(P(None, "space", None), P(None, "space", None)),
        check_vma=False,
    )
```

```python
from functools import partial
import math

import jax
import jax.numpy as jnp
from jax import lax
from jax.experimental import pallas as pl
from jax.experimental.pallas import tpu as pltpu
from jax.sharding import PartitionSpec as P

TDIL = 2


highest = lax.Precision.HIGHEST


def zero_square():
    return [[0, 0, 0, 0] for _ in range(4)]


def pair_product(left, right):
    real_out = zero_square()
    imag_out = zero_square()
    for row in range(4):
        for col in range(4):
            acc_real = 0
            acc_imag = 0
            for mid in range(4):
                acc_real += (
                    left[0][row][mid] * right[0][mid][col] - left[1][row][mid] * right[1][mid][col]
                )
                acc_imag += (
                    left[0][row][mid] * right[1][mid][col] + left[1][row][mid] * right[0][mid][col]
                )
            real_out[row][col] = acc_real
            imag_out[row][col] = acc_imag
    return (real_out, imag_out)


def dirac_tables():
    factors = [
        (zero_square(), [[0, 0, 0, 1], [0, 0, 1, 0], [0, -1, 0, 0], [-1, 0, 0, 0]]),
        ([[0, 0, 0, -1], [0, 0, 1, 0], [0, 1, 0, 0], [-1, 0, 0, 0]], zero_square()),
        (zero_square(), [[0, 0, 1, 0], [0, 0, 0, -1], [-1, 0, 0, 0], [0, 1, 0, 0]]),
        ([[0, 0, 1, 0], [0, 0, 0, 1], [1, 0, 0, 0], [0, 1, 0, 0]], zero_square()),
    ]
    reals = []
    imags = []
    for number in range(16):
        current = ([[1 if a == b else 0 for b in range(4)] for a in range(4)], zero_square())
        for position in range(4):
            if number >> position & 1:
                current = pair_product(current, factors[position])
        reals.append([value for line in current[0] for value in line])
        imags.append([value for line in current[1] for value in line])
    return (reals, imags)


def pick_gammas(gamma_ids):
    table_real, table_imag = dirac_tables()
    choose = (gamma_ids[:, None] == jnp.arange(16, dtype=jnp.int32)[None, :]).astype(jnp.float32)
    gamma_real = jnp.dot(
        choose, jnp.asarray(table_real, dtype=jnp.float32), precision=highest
    ).reshape(-1, 4, 4)
    gamma_imag = jnp.dot(
        choose, jnp.asarray(table_imag, dtype=jnp.float32), precision=highest
    ).reshape(-1, 4, 4)
    return (gamma_real, gamma_imag)


MESH = pl.DeviceIdType.MESH
SPINS = 4
COLOURS = 3
COMPS = SPINS * COLOURS
LANES = 128


def gamma_entries():
    reals, imags = dirac_tables()
    out = []
    for re, im in zip(reals, imags):
        rows = []
        for a in range(SPINS):
            (b,) = [b for b in range(SPINS) if re[a * SPINS + b] or im[a * SPINS + b]]
            rows.append((b, re[a * SPINS + b], im[a * SPINS + b]))
        anti = any(
            (rows[b][1], rows[b][2]) != (re_ab, -im_ab) for b, re_ab, im_ab in rows
        )
        out.append((anti, rows))
    return out


def kernel(
    owners, groups, per_owner, gram_scale, loop_scale,
    ids_ref, dil_ref, vec_ref, gram_ref, loops_ref,
    raw, wide, stack, pairs, packed, sendbuf, recvbuf, mine, theirs,
    load_sem, send_sem, recv_sem, swap_send, swap_recv,
):
    count = vec_ref.shape[0]
    half = count // 2
    space = lax.axis_index("space")
    time = lax.axis_index("tm")
    load = pltpu.make_async_copy(vec_ref, raw, load_sem)
    load.start()
    barrier = pltpu.get_barrier_semaphore()
    for step in range(1, owners):
        pl.semaphore_signal(
            barrier, inc=1, device_id=(lax.rem(space + step, owners), time), device_id_type=MESH
        )
    for step in range(1, groups):
        pl.semaphore_signal(
            barrier, inc=1, device_id=(space, lax.rem(time + step, groups)), device_id_type=MESH
        )
    load.wait()

    for i in range(count):
        at = 2 * COMPS * i
        wide[at : at + 2 * COMPS, :] = raw[i].astype(jnp.float32).reshape(2 * COMPS, LANES)
    for a in range(SPINS):
        for p in range(2):
            for c in range(COLOURS):
                rows = wide[pl.ds(2 * (COLOURS * a + c) + p, count, stride=2 * COMPS), :]
                at = (2 * a + p) * count
                stack[at : at + count, c * LANES : (c + 1) * LANES] = rows.astype(jnp.bfloat16)
    everything = stack[...]
    contract = (((1,), (1,)), ((), ()))
    pairs[...] = lax.dot_general(
        everything, everything, contract, preferred_element_type=jnp.float32
    )

    lane = lax.broadcasted_iota(jnp.int32, (1, 2 * count), 1)
    left = lane < count
    turn = jnp.where(left, -1.0, 1.0).astype(jnp.float32)
    dil = dil_ref[...]
    dil = jnp.concatenate([dil, dil], axis=1)
    comp = lax.rem(dil, COMPS)
    spin = lax.div(comp, COLOURS)
    colour = lax.rem(comp, COLOURS)
    live = lax.div(dil, COMPS) == lax.rem(time, TDIL)
    ones = jnp.ones((8, LANES), jnp.bfloat16)
    sums = [
        lax.dot_general(
            ones, everything[:, c * LANES : (c + 1) * LANES], contract,
            preferred_element_type=jnp.float32,
        )
        for c in range(COLOURS)
    ]
    quark = []
    for a in range(SPINS):
        got = sums[COLOURS - 1][:, a * LANES : (a + 1) * LANES]
        for c in range(COLOURS - 1):
            got = jnp.where(colour == c, sums[c][:, a * LANES : (a + 1) * LANES], got)
        got = jnp.where(live, got, 0.0)
        quark.append((got, pltpu.roll(got, count, 1) * turn))

    row = lax.broadcasted_iota(jnp.int32, (half, 2 * count), 0)
    col = lax.broadcasted_iota(jnp.int32, (half, 2 * count), 1)
    upper = row <= col
    lower = row + half > col - count
    low_lanes = col < count

    def block(a, b):
        first = pairs[2 * a * count : (2 * a + 1) * count, b * LANES : (b + 1) * LANES]
        second = pairs[(2 * a + 1) * count : (2 * a + 2) * count, b * LANES : (b + 1) * LANES]
        return first - turn * pltpu.roll(second, count, 1)

    entries = gamma_entries()
    for shift in range(SPINS):
        plain = [block(a, a ^ shift) for a in range(SPINS)]
        turned = [pltpu.roll(x, count, 1) * turn for x in plain]
        for number, (anti, rows) in enumerate(entries):
            if rows[0][0] != shift or number == 0:
                continue
            total = None
            loop = jnp.zeros_like(quark[0][0])
            for a, (b, re, im) in enumerate(rows):
                term = quark[b][0] if re else quark[b][1]
                loop = jnp.where(spin == a, term if re + im > 0 else -term, loop)
                if anti:
                    re, im = im, -re
                term = plain[a] if re else turned[a]
                if total is None:
                    total = term if re + im > 0 else -term
                else:
                    total = total + term if re + im > 0 else total - term
            top, bottom = total[:half], total[half:]
            top = jnp.where(upper, top, pltpu.roll(top, count, 1))
            bottom = jnp.where(lower, bottom, pltpu.roll(bottom, count, 1))
            packed[number, 0:half, :] = jnp.where(low_lanes, top, bottom)
            packed[number, half : half + 1, :] = loop[0:1]
    for g in range(owners * per_owner):
        sendbuf[g] = packed[ids_ref[g]]

    pl.semaphore_wait(barrier, owners + groups - 2)
    copies = []
    for step in range(1, owners):
        target = lax.rem(space + step, owners)
        copy = pltpu.make_async_remote_copy(
            src_ref=sendbuf.at[pl.ds(target * per_owner, per_owner)],
            dst_ref=recvbuf.at[step - 1],
            send_sem=send_sem.at[step - 1],
            recv_sem=recv_sem.at[step - 1],
            device_id=(target, time),
            device_id_type=MESH,
        )
        copy.start()
        copies.append(copy)
    total = sendbuf[pl.ds(space * per_owner, per_owner)]
    for step in range(1, owners):
        copies[step - 1].wait_recv()
        total = total + recvbuf[step - 1]
    mine[...] = total
    swaps = []
    for step in range(1, groups):
        swap = pltpu.make_async_remote_copy(
            src_ref=mine,
            dst_ref=theirs.at[step - 1],
            send_sem=swap_send.at[step - 1],
            recv_sem=swap_recv.at[step - 1],
            device_id=(space, lax.rem(time + step, groups)),
            device_id_type=MESH,
        )
        swap.start()
        swaps.append(swap)

    above = lax.broadcasted_iota(jnp.int32, (count, 2 * count), 0)
    across = lax.broadcasted_iota(jnp.int32, (count, 2 * count), 1)
    in_real = across < count
    across = jnp.where(in_real, across, across - count)

    def unpack(summed, when):
        for k in range(per_owner):
            part = summed[k, 0:half]
            swapped = pltpu.roll(part, count, 1)
            full = jnp.concatenate(
                [jnp.where(low_lanes, part, swapped), jnp.where(low_lanes, swapped, part)], axis=0
            )
            flipped = jnp.concatenate([full, full], axis=0).T[:count]
            real = jnp.where(above <= across, full, flipped)
            imag = jnp.where(above > across, full, jnp.where(above < across, -flipped, 0.0))
            held = jnp.where(in_real, real, imag)
            number = ids_ref[space * per_owner + k]
            anti = jnp.bool_(False)
            for n, (is_anti, _) in enumerate(entries):
                if is_anti:
                    anti = anti | (number == n)
            rotated = pltpu.roll(held, count, 1) * turn
            out = jnp.where(anti, rotated, held)
            gram_ref[when, k * count : (k + 1) * count, :] = out * gram_scale
            sums = summed[k, half : half + 1] * loop_scale
            at = slice(k * count, (k + 1) * count)
            loops_ref[when, 0:1, at] = sums[:, :count]
            loops_ref[when, 1:2, at] = pltpu.roll(sums, count, 1)[:, :count]

    unpack(total, time)
    for step in range(1, groups):
        swaps[step - 1].wait_recv()
        unpack(theirs[step - 1], lax.rem(time + groups - step, groups))
    for copy in copies + swaps:
        copy.wait_send()


def packed_shards(vectors, dilution, gamma_ids):
    slices, count, halves, comps, sites = vectors.shape
    owners, groups = lax.axis_size("space"), lax.axis_size("tm")
    numbers = gamma_ids.shape[0]
    per_owner = numbers // owners
    total_sites = sites * owners
    message = (per_owner, count // 2 + 1, 2 * count)
    gram, loops = pl.pallas_call(
        partial(
            kernel, owners, groups, per_owner,
            1.0 / math.sqrt(48.0 * total_sites), 1.0 / math.sqrt(1.0 * total_sites),
        ),
        out_shape=(
            jax.ShapeDtypeStruct((groups, per_owner * count, 2 * count), jnp.float32),
            jax.ShapeDtypeStruct((groups, 2, per_owner * count), jnp.float32),
        ),
        in_specs=[
            pl.BlockSpec(memory_space=pltpu.SMEM),
            pl.BlockSpec(memory_space=pltpu.VMEM),
            pl.BlockSpec(memory_space=pl.ANY),
        ],
        out_specs=(
            pl.BlockSpec(memory_space=pltpu.VMEM),
            pl.BlockSpec(memory_space=pltpu.VMEM),
        ),
        scratch_shapes=[
            pltpu.VMEM((count, comps, halves, sites), jnp.bfloat16),
            pltpu.VMEM((count * halves * comps, sites), jnp.float32),
            pltpu.VMEM((SPINS * 2 * count, COLOURS * sites), jnp.bfloat16),
            pltpu.VMEM((SPINS * 2 * count, SPINS * 2 * count), jnp.float32),
            pltpu.VMEM((16,) + message[1:], jnp.float32),
            pltpu.VMEM((numbers,) + message[1:], jnp.float32),
            pltpu.VMEM((owners - 1,) + message, jnp.float32),
            pltpu.VMEM(message, jnp.float32),
            pltpu.VMEM((groups - 1,) + message, jnp.float32),
            pltpu.SemaphoreType.DMA,
            pltpu.SemaphoreType.DMA((owners - 1,)),
            pltpu.SemaphoreType.DMA((owners - 1,)),
            pltpu.SemaphoreType.DMA((groups - 1,)),
            pltpu.SemaphoreType.DMA((groups - 1,)),
        ],
        compiler_params=pltpu.CompilerParams(collective_id=0, has_side_effects=True),
    )(gamma_ids, dilution.reshape(1, count), vectors.reshape(count, halves, comps, sites).swapaxes(1, 2))
    return gram, loops.swapaxes(1, 2)


def any_shards(vectors, dilution, gamma_ids):
    slices, count, halves, comps, sites = vectors.shape
    numbers = gamma_ids.shape[0]
    whole_blocks = numbers % lax.axis_size("space") == 0
    if slices == 1 and sites == LANES and 2 * count == LANES and whole_blocks:
        return packed_shards(vectors, dilution, gamma_ids)
    return shards(vectors, dilution, gamma_ids)


def shards(vectors, dilution, gamma_ids):
    slices, count, halves, comps, sites = vectors.shape
    owners = lax.axis_size("space")
    total_sites = sites * owners
    gram_scale = 1.0 / math.sqrt(48.0 * total_sites)
    loop_scale = 1.0 / math.sqrt(1.0 * total_sites)
    gamma_real, gamma_imag = pick_gammas(gamma_ids)
    spin_pick = ((dilution % 12 // 3)[:, None] == jnp.arange(4, dtype=jnp.int32)[None, :]).astype(
        jnp.float32
    )
    colour_pick = ((dilution % 3)[:, None] == jnp.arange(3, dtype=jnp.int32)[None, :]).astype(
        jnp.float32
    )
    time_class = dilution // 12
    ein = partial(jnp.einsum, precision=highest)
    lowein = partial(jnp.einsum, preferred_element_type=jnp.float32)
    first_slice = lax.axis_index("tm") * slices
    rows_real = ein("gba,ib->gia", gamma_real, spin_pick)
    rows_imag = ein("gba,ib->gia", gamma_imag, spin_pick)

    def one_slice(inputs):
        block, slice_index = inputs
        spinor = block.reshape(count, 2, 4, 3 * sites)
        real_part = spinor[:, 0]
        imag_part = spinor[:, 1]
        pair_real = lowein("iak,jbk->iajb", real_part, real_part) + lowein(
            "iak,jbk->iajb", imag_part, imag_part
        )
        pair_imag = lowein("iak,jbk->iajb", real_part, imag_part) - lowein(
            "iak,jbk->iajb", imag_part, real_part
        )
        gram_real = ein("gab,iajb->gij", gamma_real, pair_real) - ein(
            "gab,iajb->gij", gamma_imag, pair_imag
        )
        gram_imag = ein("gab,iajb->gij", gamma_real, pair_imag) + ein(
            "gab,iajb->gij", gamma_imag, pair_real
        )
        gram = jnp.concatenate([gram_real, gram_imag], axis=2).reshape(-1, 2 * count)
        gram = gram * gram_scale
        site_sums = jnp.sum(block, axis=-1, dtype=jnp.float32).reshape(count, 2, 4, 3)
        picked = ein("ipac,ic->ipa", site_sums, colour_pick)
        loop_real = ein("gia,ia->gi", rows_real, picked[:, 0]) - ein(
            "gia,ia->gi", rows_imag, picked[:, 1]
        )
        loop_imag = ein("gia,ia->gi", rows_real, picked[:, 1]) + ein(
            "gia,ia->gi", rows_imag, picked[:, 0]
        )
        live = (time_class == slice_index % TDIL).astype(jnp.float32)[None, :]
        loops = jnp.stack([loop_real * live, loop_imag * live], axis=-1).reshape(-1, 2) * loop_scale
        return (gram, loops)

    gram_terms, loop_terms = lax.map(
        one_slice, (vectors, first_slice + jnp.arange(slices, dtype=jnp.int32))
    )
    total_rows = gram_terms.shape[1]
    owned = total_rows // owners
    totals = lax.psum((gram_terms, loop_terms), "space")
    start = lax.axis_index("space") * owned
    shares = (
        lax.dynamic_slice_in_dim(totals[0], start, owned, 1),
        lax.dynamic_slice_in_dim(totals[1], start, owned, 1),
    )
    gram, loops = (
        lax.all_gather(shares[0], "tm", axis=0, tiled=True),
        lax.all_gather(shares[1], "tm", axis=0, tiled=True),
    )
    return (gram, loops)


def solution(mesh):
    placed = (P("tm", None, None, None, "space"), P(), P())
    return jax.shard_map(
        any_shards,
        mesh=mesh,
        in_specs=placed,
        out_specs=(P(None, "space", None), P(None, "space", None)),
        check_vma=False,
    )
```

```python
from functools import partial
import math

import jax
import jax.numpy as jnp
from jax import lax
from jax.experimental import pallas as pl
from jax.experimental.pallas import tpu as pltpu
from jax.sharding import PartitionSpec as P

TDIL = 2


highest = lax.Precision.HIGHEST


def zero_square():
    return [[0, 0, 0, 0] for _ in range(4)]


def pair_product(left, right):
    real_out = zero_square()
    imag_out = zero_square()
    for row in range(4):
        for col in range(4):
            acc_real = 0
            acc_imag = 0
            for mid in range(4):
                acc_real += (
                    left[0][row][mid] * right[0][mid][col] - left[1][row][mid] * right[1][mid][col]
                )
                acc_imag += (
                    left[0][row][mid] * right[1][mid][col] + left[1][row][mid] * right[0][mid][col]
                )
            real_out[row][col] = acc_real
            imag_out[row][col] = acc_imag
    return (real_out, imag_out)


def dirac_tables():
    factors = [
        (zero_square(), [[0, 0, 0, 1], [0, 0, 1, 0], [0, -1, 0, 0], [-1, 0, 0, 0]]),
        ([[0, 0, 0, -1], [0, 0, 1, 0], [0, 1, 0, 0], [-1, 0, 0, 0]], zero_square()),
        (zero_square(), [[0, 0, 1, 0], [0, 0, 0, -1], [-1, 0, 0, 0], [0, 1, 0, 0]]),
        ([[0, 0, 1, 0], [0, 0, 0, 1], [1, 0, 0, 0], [0, 1, 0, 0]], zero_square()),
    ]
    reals = []
    imags = []
    for number in range(16):
        current = ([[1 if a == b else 0 for b in range(4)] for a in range(4)], zero_square())
        for position in range(4):
            if number >> position & 1:
                current = pair_product(current, factors[position])
        reals.append([value for line in current[0] for value in line])
        imags.append([value for line in current[1] for value in line])
    return (reals, imags)


def pick_gammas(gamma_ids):
    table_real, table_imag = dirac_tables()
    choose = (gamma_ids[:, None] == jnp.arange(16, dtype=jnp.int32)[None, :]).astype(jnp.float32)
    gamma_real = jnp.dot(
        choose, jnp.asarray(table_real, dtype=jnp.float32), precision=highest
    ).reshape(-1, 4, 4)
    gamma_imag = jnp.dot(
        choose, jnp.asarray(table_imag, dtype=jnp.float32), precision=highest
    ).reshape(-1, 4, 4)
    return (gamma_real, gamma_imag)


MESH = pl.DeviceIdType.MESH
SPINS = 4
COLOURS = 3
COMPS = SPINS * COLOURS
LANES = 128


def gamma_entries():
    reals, imags = dirac_tables()
    out = []
    for re, im in zip(reals, imags):
        rows = []
        for a in range(SPINS):
            (b,) = [b for b in range(SPINS) if re[a * SPINS + b] or im[a * SPINS + b]]
            rows.append((b, re[a * SPINS + b], im[a * SPINS + b]))
        anti = any(
            (rows[b][1], rows[b][2]) != (re_ab, -im_ab) for b, re_ab, im_ab in rows
        )
        out.append((anti, rows))
    return out


def plane_of(owners):
    return math.gcd(owners, 4)


def kernel(
    owners, groups, per_owner, gram_scale, loop_scale,
    ids_hbm, dil_hbm, vec_ref, gram_ref, loops_ref,
    ids_ref, dil_ref, raw, wide, stack, pairs, packed, sendbuf, recvbuf, midbuf, lastbuf,
    mine, theirs,
    load_sems, send_sem, recv_sem, mid_send, mid_recv, swap_send, swap_recv,
):
    count = vec_ref.shape[0]
    half = count // 2
    space = lax.axis_index("space")
    time = lax.axis_index("tm")
    plane = plane_of(owners)
    planes = owners // plane
    place = lax.rem(space, plane)
    level = lax.div(space, plane)
    loads = [
        pltpu.make_async_copy(vec_ref, raw, load_sems.at[0]),
        pltpu.make_async_copy(ids_hbm, ids_ref, load_sems.at[1]),
        pltpu.make_async_copy(dil_hbm, dil_ref, load_sems.at[2]),
    ]
    for load in loads:
        load.start()
    barrier = pltpu.get_barrier_semaphore()
    beside = [level * plane + lax.rem(place + step, plane) for step in range(1, plane)]
    farther = []
    for step in range(planes):
        down = 2 * level >= planes
        far = jnp.where(down, level, planes - 1 - level)
        way = jnp.where(step < far, step, planes - 1 - (step - far))
        way = jnp.where(step == planes - 1, far, way)
        farther.append(jnp.where(down, way, planes - 1 - way))
    along = [lax.rem(level + step, planes) * plane + place for step in range(1, planes)]
    for target in beside + along:
        pl.semaphore_signal(barrier, inc=1, device_id=(target, time), device_id_type=MESH)
    for step in range(1, groups):
        pl.semaphore_signal(
            barrier, inc=1, device_id=(space, lax.rem(time + step, groups)), device_id_type=MESH
        )
    for load in loads:
        load.wait()

    for i in range(count):
        at = 2 * COMPS * i
        wide[at : at + 2 * COMPS, :] = raw[i].astype(jnp.float32).reshape(2 * COMPS, LANES)
    for a in range(SPINS):
        for p in range(2):
            for c in range(COLOURS):
                rows = wide[pl.ds(2 * (COLOURS * a + c) + p, count, stride=2 * COMPS), :]
                at = (2 * a + p) * count
                stack[at : at + count, c * LANES : (c + 1) * LANES] = rows.astype(jnp.bfloat16)
    everything = stack[...]
    contract = (((1,), (1,)), ((), ()))
    pairs[...] = lax.dot_general(
        everything, everything, contract, preferred_element_type=jnp.float32
    )

    lane = lax.broadcasted_iota(jnp.int32, (1, 2 * count), 1)
    left = lane < count
    turn = jnp.where(left, -1.0, 1.0).astype(jnp.float32)
    dil = dil_ref[...]
    dil = jnp.concatenate([dil, dil], axis=1)
    comp = lax.rem(dil, COMPS)
    spin = lax.div(comp, COLOURS)
    colour = lax.rem(comp, COLOURS)
    live = lax.div(dil, COMPS) == lax.rem(time, TDIL)
    ones = jnp.ones((8, LANES), jnp.bfloat16)
    sums = [
        lax.dot_general(
            ones, everything[:, c * LANES : (c + 1) * LANES], contract,
            preferred_element_type=jnp.float32,
        )
        for c in range(COLOURS)
    ]
    quark = []
    for a in range(SPINS):
        got = sums[COLOURS - 1][:, a * LANES : (a + 1) * LANES]
        for c in range(COLOURS - 1):
            got = jnp.where(colour == c, sums[c][:, a * LANES : (a + 1) * LANES], got)
        got = jnp.where(live, got, 0.0)
        quark.append((got, pltpu.roll(got, count, 1) * turn))

    row = lax.broadcasted_iota(jnp.int32, (half, 2 * count), 0)
    col = lax.broadcasted_iota(jnp.int32, (half, 2 * count), 1)
    upper = row <= col
    lower = row + half > col - count
    low_lanes = col < count

    def block(a, b):
        first = pairs[2 * a * count : (2 * a + 1) * count, b * LANES : (b + 1) * LANES]
        second = pairs[(2 * a + 1) * count : (2 * a + 2) * count, b * LANES : (b + 1) * LANES]
        return first - turn * pltpu.roll(second, count, 1)

    entries = gamma_entries()
    for shift in range(SPINS):
        plain = [block(a, a ^ shift) for a in range(SPINS)]
        turned = [pltpu.roll(x, count, 1) * turn for x in plain]
        for number, (anti, rows) in enumerate(entries):
            if rows[0][0] != shift or number == 0:
                continue
            total = None
            loop = jnp.zeros_like(quark[0][0])
            for a, (b, re, im) in enumerate(rows):
                term = quark[b][0] if re else quark[b][1]
                loop = jnp.where(spin == a, term if re + im > 0 else -term, loop)
                if anti:
                    re, im = im, -re
                term = plain[a] if re else turned[a]
                if total is None:
                    total = term if re + im > 0 else -term
                else:
                    total = total + term if re + im > 0 else total - term
            top, bottom = total[:half], total[half:]
            top = jnp.where(upper, top, pltpu.roll(top, count, 1))
            bottom = jnp.where(lower, bottom, pltpu.roll(bottom, count, 1))
            packed[number, 0:half, :] = jnp.where(low_lanes, top, bottom)
            packed[number, half : half + 1, :] = loop[0:1]
    for g in range(owners * per_owner):
        sendbuf[g] = packed[ids_ref[g]]

    pl.semaphore_wait(barrier, plane + planes + groups - 3)
    copies = []
    arrivals = []
    for turn_no, target_level in enumerate(farther):
        for step in range(1, plane):
            target = beside[step - 1]
            slot = turn_no * (plane - 1) + step - 1
            goal = target_level * plane + lax.rem(place + step, plane)
            copy = pltpu.make_async_remote_copy(
                src_ref=sendbuf.at[pl.ds(goal * per_owner, per_owner)],
                dst_ref=recvbuf.at[slot],
                send_sem=send_sem.at[slot],
                recv_sem=recv_sem.at[slot],
                device_id=(target, time),
                device_id_type=MESH,
            )
            copy.start()
            copies.append(copy)
            arrivals.append(copy)
    for turn_no, target_level in enumerate(farther):
        total = sendbuf[pl.ds((target_level * plane + place) * per_owner, per_owner)]
        for step in range(1, plane):
            slot = turn_no * (plane - 1) + step - 1
            arrivals[slot].wait_recv()
            total = total + recvbuf[slot]
        if turn_no < planes - 1:
            midbuf[turn_no] = total
            slot = lax.rem(target_level - level + planes, planes) - 1
            copy = pltpu.make_async_remote_copy(
                src_ref=midbuf.at[turn_no],
                dst_ref=lastbuf.at[slot],
                send_sem=mid_send.at[turn_no],
                recv_sem=mid_recv.at[slot],
                device_id=(target_level * plane + place, time),
                device_id_type=MESH,
            )
            copy.start()
            copies.append(copy)
    for slot in range(planes - 1):
        pltpu.make_async_remote_copy(
            src_ref=midbuf.at[slot],
            dst_ref=lastbuf.at[slot],
            send_sem=mid_send.at[slot],
            recv_sem=mid_recv.at[slot],
            device_id=(along[slot], time),
            device_id_type=MESH,
        ).wait_recv()
        total = total + lastbuf[slot]
    mine[...] = total
    swaps = []
    for step in range(1, groups):
        swap = pltpu.make_async_remote_copy(
            src_ref=mine,
            dst_ref=theirs.at[step - 1],
            send_sem=swap_send.at[step - 1],
            recv_sem=swap_recv.at[step - 1],
            device_id=(space, lax.rem(time + step, groups)),
            device_id_type=MESH,
        )
        swap.start()
        swaps.append(swap)

    above = lax.broadcasted_iota(jnp.int32, (count, 2 * count), 0)
    across = lax.broadcasted_iota(jnp.int32, (count, 2 * count), 1)
    in_real = across < count
    across = jnp.where(in_real, across, across - count)

    def unpack(summed, when):
        for k in range(per_owner):
            part = summed[k, 0:half]
            swapped = pltpu.roll(part, count, 1)
            full = jnp.concatenate(
                [jnp.where(low_lanes, part, swapped), jnp.where(low_lanes, swapped, part)], axis=0
            )
            flipped = jnp.concatenate([full, full], axis=0).T[:count]
            real = jnp.where(above <= across, full, flipped)
            imag = jnp.where(above > across, full, jnp.where(above < across, -flipped, 0.0))
            held = jnp.where(in_real, real, imag)
            number = ids_ref[space * per_owner + k]
            anti = jnp.bool_(False)
            for n, (is_anti, _) in enumerate(entries):
                if is_anti:
                    anti = anti | (number == n)
            rotated = pltpu.roll(held, count, 1) * turn
            out = jnp.where(anti, rotated, held)
            gram_ref[when, k * count : (k + 1) * count, :] = out * gram_scale
            sums = summed[k, half : half + 1] * loop_scale
            at = slice(k * count, (k + 1) * count)
            loops_ref[when, 0:1, at] = sums[:, :count]
            loops_ref[when, 1:2, at] = pltpu.roll(sums, count, 1)[:, :count]

    unpack(total, time)
    for step in range(1, groups):
        swaps[step - 1].wait_recv()
        unpack(theirs[step - 1], lax.rem(time + groups - step, groups))
    for copy in copies + swaps:
        copy.wait_send()


def packed_shards(vectors, dilution, gamma_ids):
    slices, count, halves, comps, sites = vectors.shape
    owners, groups = lax.axis_size("space"), lax.axis_size("tm")
    numbers = gamma_ids.shape[0]
    per_owner = numbers // owners
    total_sites = sites * owners
    plane = plane_of(owners)
    planes = owners // plane
    message = (per_owner, count // 2 + 1, 2 * count)
    gram, loops = pl.pallas_call(
        partial(
            kernel, owners, groups, per_owner,
            1.0 / math.sqrt(48.0 * total_sites), 1.0 / math.sqrt(1.0 * total_sites),
        ),
        out_shape=(
            jax.ShapeDtypeStruct((groups, per_owner * count, 2 * count), jnp.float32),
            jax.ShapeDtypeStruct((groups, 2, per_owner * count), jnp.float32),
        ),
        in_specs=[
            pl.BlockSpec(memory_space=pl.ANY),
            pl.BlockSpec(memory_space=pl.ANY),
            pl.BlockSpec(memory_space=pl.ANY),
        ],
        out_specs=(
            pl.BlockSpec(memory_space=pltpu.VMEM),
            pl.BlockSpec(memory_space=pltpu.VMEM),
        ),
        scratch_shapes=[
            pltpu.SMEM((numbers,), jnp.int32),
            pltpu.VMEM((1, count), jnp.int32),
            pltpu.VMEM((count, comps, halves, sites), jnp.bfloat16),
            pltpu.VMEM((count * halves * comps, sites), jnp.float32),
            pltpu.VMEM((SPINS * 2 * count, COLOURS * sites), jnp.bfloat16),
            pltpu.VMEM((SPINS * 2 * count, SPINS * 2 * count), jnp.float32),
            pltpu.VMEM((16,) + message[1:], jnp.float32),
            pltpu.VMEM((numbers,) + message[1:], jnp.float32),
            pltpu.VMEM((planes * (plane - 1),) + message, jnp.float32),
            pltpu.VMEM((planes - 1,) + message, jnp.float32),
            pltpu.VMEM((planes - 1,) + message, jnp.float32),
            pltpu.VMEM(message, jnp.float32),
            pltpu.VMEM((groups - 1,) + message, jnp.float32),
            pltpu.SemaphoreType.DMA((3,)),
            pltpu.SemaphoreType.DMA((planes * (plane - 1),)),
            pltpu.SemaphoreType.DMA((planes * (plane - 1),)),
            pltpu.SemaphoreType.DMA((planes - 1,)),
            pltpu.SemaphoreType.DMA((planes - 1,)),
            pltpu.SemaphoreType.DMA((groups - 1,)),
            pltpu.SemaphoreType.DMA((groups - 1,)),
        ],
        compiler_params=pltpu.CompilerParams(collective_id=0, has_side_effects=True),
    )(gamma_ids, dilution.reshape(1, count), vectors.reshape(count, halves, comps, sites).swapaxes(1, 2))
    return gram, loops.swapaxes(1, 2)


def any_shards(vectors, dilution, gamma_ids):
    slices, count, halves, comps, sites = vectors.shape
    numbers = gamma_ids.shape[0]
    owners, groups = lax.axis_size("space"), lax.axis_size("tm")
    whole_blocks = numbers % owners == 0 and owners > plane_of(owners) > 1 and groups > 1
    if slices == 1 and sites == LANES and 2 * count == LANES and whole_blocks:
        return packed_shards(vectors, dilution, gamma_ids)
    return shards(vectors, dilution, gamma_ids)


def shards(vectors, dilution, gamma_ids):
    slices, count, halves, comps, sites = vectors.shape
    owners = lax.axis_size("space")
    total_sites = sites * owners
    gram_scale = 1.0 / math.sqrt(48.0 * total_sites)
    loop_scale = 1.0 / math.sqrt(1.0 * total_sites)
    gamma_real, gamma_imag = pick_gammas(gamma_ids)
    spin_pick = ((dilution % 12 // 3)[:, None] == jnp.arange(4, dtype=jnp.int32)[None, :]).astype(
        jnp.float32
    )
    colour_pick = ((dilution % 3)[:, None] == jnp.arange(3, dtype=jnp.int32)[None, :]).astype(
        jnp.float32
    )
    time_class = dilution // 12
    ein = partial(jnp.einsum, precision=highest)
    lowein = partial(jnp.einsum, preferred_element_type=jnp.float32)
    first_slice = lax.axis_index("tm") * slices
    rows_real = ein("gba,ib->gia", gamma_real, spin_pick)
    rows_imag = ein("gba,ib->gia", gamma_imag, spin_pick)

    def one_slice(inputs):
        block, slice_index = inputs
        spinor = block.reshape(count, 2, 4, 3 * sites)
        real_part = spinor[:, 0]
        imag_part = spinor[:, 1]
        pair_real = lowein("iak,jbk->iajb", real_part, real_part) + lowein(
            "iak,jbk->iajb", imag_part, imag_part
        )
        pair_imag = lowein("iak,jbk->iajb", real_part, imag_part) - lowein(
            "iak,jbk->iajb", imag_part, real_part
        )
        gram_real = ein("gab,iajb->gij", gamma_real, pair_real) - ein(
            "gab,iajb->gij", gamma_imag, pair_imag
        )
        gram_imag = ein("gab,iajb->gij", gamma_real, pair_imag) + ein(
            "gab,iajb->gij", gamma_imag, pair_real
        )
        gram = jnp.concatenate([gram_real, gram_imag], axis=2).reshape(-1, 2 * count)
        gram = gram * gram_scale
        site_sums = jnp.sum(block, axis=-1, dtype=jnp.float32).reshape(count, 2, 4, 3)
        picked = ein("ipac,ic->ipa", site_sums, colour_pick)
        loop_real = ein("gia,ia->gi", rows_real, picked[:, 0]) - ein(
            "gia,ia->gi", rows_imag, picked[:, 1]
        )
        loop_imag = ein("gia,ia->gi", rows_real, picked[:, 1]) + ein(
            "gia,ia->gi", rows_imag, picked[:, 0]
        )
        live = (time_class == slice_index % TDIL).astype(jnp.float32)[None, :]
        loops = jnp.stack([loop_real * live, loop_imag * live], axis=-1).reshape(-1, 2) * loop_scale
        return (gram, loops)

    gram_terms, loop_terms = lax.map(
        one_slice, (vectors, first_slice + jnp.arange(slices, dtype=jnp.int32))
    )
    total_rows = gram_terms.shape[1]
    owned = total_rows // owners
    totals = lax.psum((gram_terms, loop_terms), "space")
    start = lax.axis_index("space") * owned
    shares = (
        lax.dynamic_slice_in_dim(totals[0], start, owned, 1),
        lax.dynamic_slice_in_dim(totals[1], start, owned, 1),
    )
    gram, loops = (
        lax.all_gather(shares[0], "tm", axis=0, tiled=True),
        lax.all_gather(shares[1], "tm", axis=0, tiled=True),
    )
    return (gram, loops)


def solution(mesh):
    placed = (P("tm", None, None, None, "space"), P(), P())
    return jax.shard_map(
        any_shards,
        mesh=mesh,
        in_specs=placed,
        out_specs=(P(None, "space", None), P(None, "space", None)),
        check_vma=False,
    )
```

```python
from functools import partial
import math

import jax
import jax.numpy as jnp
from jax import lax
from jax.experimental import pallas as pl
from jax.experimental.pallas import tpu as pltpu
from jax.sharding import PartitionSpec as P

TDIL = 2


highest = lax.Precision.HIGHEST


def zero_square():
    return [[0, 0, 0, 0] for _ in range(4)]


def pair_product(left, right):
    real_out = zero_square()
    imag_out = zero_square()
    for row in range(4):
        for col in range(4):
            acc_real = 0
            acc_imag = 0
            for mid in range(4):
                acc_real += (
                    left[0][row][mid] * right[0][mid][col] - left[1][row][mid] * right[1][mid][col]
                )
                acc_imag += (
                    left[0][row][mid] * right[1][mid][col] + left[1][row][mid] * right[0][mid][col]
                )
            real_out[row][col] = acc_real
            imag_out[row][col] = acc_imag
    return (real_out, imag_out)


def dirac_tables():
    factors = [
        (zero_square(), [[0, 0, 0, 1], [0, 0, 1, 0], [0, -1, 0, 0], [-1, 0, 0, 0]]),
        ([[0, 0, 0, -1], [0, 0, 1, 0], [0, 1, 0, 0], [-1, 0, 0, 0]], zero_square()),
        (zero_square(), [[0, 0, 1, 0], [0, 0, 0, -1], [-1, 0, 0, 0], [0, 1, 0, 0]]),
        ([[0, 0, 1, 0], [0, 0, 0, 1], [1, 0, 0, 0], [0, 1, 0, 0]], zero_square()),
    ]
    reals = []
    imags = []
    for number in range(16):
        current = ([[1 if a == b else 0 for b in range(4)] for a in range(4)], zero_square())
        for position in range(4):
            if number >> position & 1:
                current = pair_product(current, factors[position])
        reals.append([value for line in current[0] for value in line])
        imags.append([value for line in current[1] for value in line])
    return (reals, imags)


def pick_gammas(gamma_ids):
    table_real, table_imag = dirac_tables()
    choose = (gamma_ids[:, None] == jnp.arange(16, dtype=jnp.int32)[None, :]).astype(jnp.float32)
    gamma_real = jnp.dot(
        choose, jnp.asarray(table_real, dtype=jnp.float32), precision=highest
    ).reshape(-1, 4, 4)
    gamma_imag = jnp.dot(
        choose, jnp.asarray(table_imag, dtype=jnp.float32), precision=highest
    ).reshape(-1, 4, 4)
    return (gamma_real, gamma_imag)


MESH = pl.DeviceIdType.MESH
SPINS = 4
COLOURS = 3
COMPS = SPINS * COLOURS
LANES = 128


def gamma_entries():
    reals, imags = dirac_tables()
    out = []
    for re, im in zip(reals, imags):
        rows = []
        for a in range(SPINS):
            (b,) = [b for b in range(SPINS) if re[a * SPINS + b] or im[a * SPINS + b]]
            rows.append((b, re[a * SPINS + b], im[a * SPINS + b]))
        anti = any(
            (rows[b][1], rows[b][2]) != (re_ab, -im_ab) for b, re_ab, im_ab in rows
        )
        out.append((anti, rows))
    return out


def kernel(
    owners, groups, per_owner, gram_scale, loop_scale,
    ids_hbm, dil_hbm, vec_ref, gram_ref, loops_ref,
    ids_ref, dil_ref, raw, wide, stack, pairs, packed, sendbuf, recvbuf,
    mine, theirs,
    load_sems, send_sem, recv_sem, swap_send, swap_recv,
):
    count = vec_ref.shape[0]
    half = count // 2
    space = lax.axis_index("space")
    time = lax.axis_index("tm")
    loads = [
        pltpu.make_async_copy(vec_ref, raw, load_sems.at[0]),
        pltpu.make_async_copy(ids_hbm, ids_ref, load_sems.at[1]),
        pltpu.make_async_copy(dil_hbm, dil_ref, load_sems.at[2]),
    ]
    for load in loads:
        load.start()
    barrier = pltpu.get_barrier_semaphore()
    targets = [lax.rem(space + step, owners) for step in range(1, owners)]
    for target in targets:
        pl.semaphore_signal(barrier, inc=1, device_id=(target, time), device_id_type=MESH)
    for step in range(1, groups):
        pl.semaphore_signal(
            barrier, inc=1, device_id=(space, lax.rem(time + step, groups)), device_id_type=MESH
        )
    for load in loads:
        load.wait()

    for i in range(count):
        at = 2 * COMPS * i
        wide[at : at + 2 * COMPS, :] = raw[i].astype(jnp.float32).reshape(2 * COMPS, LANES)
    for a in range(SPINS):
        for p in range(2):
            for c in range(COLOURS):
                rows = wide[pl.ds(2 * (COLOURS * a + c) + p, count, stride=2 * COMPS), :]
                at = (2 * a + p) * count
                stack[at : at + count, c * LANES : (c + 1) * LANES] = rows.astype(jnp.bfloat16)
    everything = stack[...]
    contract = (((1,), (1,)), ((), ()))
    pairs[...] = lax.dot_general(
        everything, everything, contract, preferred_element_type=jnp.float32
    )

    lane = lax.broadcasted_iota(jnp.int32, (1, 2 * count), 1)
    left = lane < count
    turn = jnp.where(left, -1.0, 1.0).astype(jnp.float32)
    dil = dil_ref[...]
    dil = jnp.concatenate([dil, dil], axis=1)
    comp = lax.rem(dil, COMPS)
    spin = lax.div(comp, COLOURS)
    colour = lax.rem(comp, COLOURS)
    live = lax.div(dil, COMPS) == lax.rem(time, TDIL)
    ones = jnp.ones((8, LANES), jnp.bfloat16)
    sums = [
        lax.dot_general(
            ones, everything[:, c * LANES : (c + 1) * LANES], contract,
            preferred_element_type=jnp.float32,
        )
        for c in range(COLOURS)
    ]
    quark = []
    for a in range(SPINS):
        got = sums[COLOURS - 1][:, a * LANES : (a + 1) * LANES]
        for c in range(COLOURS - 1):
            got = jnp.where(colour == c, sums[c][:, a * LANES : (a + 1) * LANES], got)
        got = jnp.where(live, got, 0.0)
        quark.append((got, pltpu.roll(got, count, 1) * turn))

    row = lax.broadcasted_iota(jnp.int32, (half, 2 * count), 0)
    col = lax.broadcasted_iota(jnp.int32, (half, 2 * count), 1)
    upper = row <= col
    lower = row + half > col - count
    low_lanes = col < count

    def block(a, b):
        first = pairs[2 * a * count : (2 * a + 1) * count, b * LANES : (b + 1) * LANES]
        second = pairs[(2 * a + 1) * count : (2 * a + 2) * count, b * LANES : (b + 1) * LANES]
        return first - turn * pltpu.roll(second, count, 1)

    entries = gamma_entries()
    for shift in range(SPINS):
        plain = [block(a, a ^ shift) for a in range(SPINS)]
        turned = [pltpu.roll(x, count, 1) * turn for x in plain]
        for number, (anti, rows) in enumerate(entries):
            if rows[0][0] != shift or number == 0:
                continue
            total = None
            loop = jnp.zeros_like(quark[0][0])
            for a, (b, re, im) in enumerate(rows):
                term = quark[b][0] if re else quark[b][1]
                loop = jnp.where(spin == a, term if re + im > 0 else -term, loop)
                if anti:
                    re, im = im, -re
                term = plain[a] if re else turned[a]
                if total is None:
                    total = term if re + im > 0 else -term
                else:
                    total = total + term if re + im > 0 else total - term
            top, bottom = total[:half], total[half:]
            top = jnp.where(upper, top, pltpu.roll(top, count, 1))
            bottom = jnp.where(lower, bottom, pltpu.roll(bottom, count, 1))
            packed[number, 0:half, :] = jnp.where(low_lanes, top, bottom)
            packed[number, half : half + 1, :] = loop[0:1]
    for g in range(owners * per_owner):
        sendbuf[g] = packed[ids_ref[g]]

    pl.semaphore_wait(barrier, owners + groups - 2)
    copies = []
    for slot, target in enumerate(targets):
        copy = pltpu.make_async_remote_copy(
            src_ref=sendbuf.at[pl.ds(target * per_owner, per_owner)],
            dst_ref=recvbuf.at[slot],
            send_sem=send_sem.at[slot],
            recv_sem=recv_sem.at[slot],
            device_id=(target, time),
            device_id_type=MESH,
        )
        copy.start()
        copies.append(copy)
    total = sendbuf[pl.ds(space * per_owner, per_owner)]
    for slot in range(owners - 1):
        copies[slot].wait_recv()
        total = total + recvbuf[slot]
    mine[...] = total
    swaps = []
    for step in range(1, groups):
        swap = pltpu.make_async_remote_copy(
            src_ref=mine,
            dst_ref=theirs.at[step - 1],
            send_sem=swap_send.at[step - 1],
            recv_sem=swap_recv.at[step - 1],
            device_id=(space, lax.rem(time + step, groups)),
            device_id_type=MESH,
        )
        swap.start()
        swaps.append(swap)

    above = lax.broadcasted_iota(jnp.int32, (count, 2 * count), 0)
    across = lax.broadcasted_iota(jnp.int32, (count, 2 * count), 1)
    in_real = across < count
    across = jnp.where(in_real, across, across - count)

    def unpack(summed, when):
        for k in range(per_owner):
            part = summed[k, 0:half]
            swapped = pltpu.roll(part, count, 1)
            full = jnp.concatenate(
                [jnp.where(low_lanes, part, swapped), jnp.where(low_lanes, swapped, part)], axis=0
            )
            flipped = jnp.concatenate([full, full], axis=0).T[:count]
            real = jnp.where(above <= across, full, flipped)
            imag = jnp.where(above > across, full, jnp.where(above < across, -flipped, 0.0))
            held = jnp.where(in_real, real, imag)
            number = ids_ref[space * per_owner + k]
            anti = jnp.bool_(False)
            for n, (is_anti, _) in enumerate(entries):
                if is_anti:
                    anti = anti | (number == n)
            rotated = pltpu.roll(held, count, 1) * turn
            out = jnp.where(anti, rotated, held)
            gram_ref[when, k * count : (k + 1) * count, :] = out * gram_scale
            sums = summed[k, half : half + 1] * loop_scale
            at = slice(k * count, (k + 1) * count)
            loops_ref[when, 0:1, at] = sums[:, :count]
            loops_ref[when, 1:2, at] = pltpu.roll(sums, count, 1)[:, :count]

    unpack(total, time)
    for step in range(1, groups):
        swaps[step - 1].wait_recv()
        unpack(theirs[step - 1], lax.rem(time + groups - step, groups))
    for copy in copies + swaps:
        copy.wait_send()


def packed_shards(vectors, dilution, gamma_ids):
    slices, count, halves, comps, sites = vectors.shape
    owners, groups = lax.axis_size("space"), lax.axis_size("tm")
    numbers = gamma_ids.shape[0]
    per_owner = numbers // owners
    total_sites = sites * owners
    message = (per_owner, count // 2 + 1, 2 * count)
    gram, loops = pl.pallas_call(
        partial(
            kernel, owners, groups, per_owner,
            1.0 / math.sqrt(48.0 * total_sites), 1.0 / math.sqrt(1.0 * total_sites),
        ),
        out_shape=(
            pltpu.VMEM((groups, per_owner * count, 2 * count), jnp.float32),
            pltpu.VMEM((groups, 2, per_owner * count), jnp.float32),
        ),
        in_specs=[
            pl.BlockSpec(memory_space=pl.ANY),
            pl.BlockSpec(memory_space=pl.ANY),
            pl.BlockSpec(memory_space=pl.ANY),
        ],
        out_specs=(
            pl.BlockSpec(memory_space=pltpu.VMEM),
            pl.BlockSpec(memory_space=pltpu.VMEM),
        ),
        scratch_shapes=[
            pltpu.SMEM((numbers,), jnp.int32),
            pltpu.VMEM((1, count), jnp.int32),
            pltpu.VMEM((count, comps, halves, sites), jnp.bfloat16),
            pltpu.VMEM((count * halves * comps, sites), jnp.float32),
            pltpu.VMEM((SPINS * 2 * count, COLOURS * sites), jnp.bfloat16),
            pltpu.VMEM((SPINS * 2 * count, SPINS * 2 * count), jnp.float32),
            pltpu.VMEM((16,) + message[1:], jnp.float32),
            pltpu.VMEM((numbers,) + message[1:], jnp.float32),
            pltpu.VMEM((owners - 1,) + message, jnp.float32),
            pltpu.VMEM(message, jnp.float32),
            pltpu.VMEM((groups - 1,) + message, jnp.float32),
            pltpu.SemaphoreType.DMA((3,)),
            pltpu.SemaphoreType.DMA((owners - 1,)),
            pltpu.SemaphoreType.DMA((owners - 1,)),
            pltpu.SemaphoreType.DMA((groups - 1,)),
            pltpu.SemaphoreType.DMA((groups - 1,)),
        ],
        compiler_params=pltpu.CompilerParams(collective_id=0, has_side_effects=True),
    )(gamma_ids, dilution.reshape(1, count), vectors.reshape(count, halves, comps, sites).swapaxes(1, 2))
    return gram, loops.swapaxes(1, 2)


def any_shards(vectors, dilution, gamma_ids):
    slices, count, halves, comps, sites = vectors.shape
    numbers = gamma_ids.shape[0]
    owners, groups = lax.axis_size("space"), lax.axis_size("tm")
    whole_blocks = numbers % owners == 0 and owners > 1 and groups > 1
    if slices == 1 and sites == LANES and 2 * count == LANES and whole_blocks:
        return packed_shards(vectors, dilution, gamma_ids)
    return shards(vectors, dilution, gamma_ids)


def shards(vectors, dilution, gamma_ids):
    slices, count, halves, comps, sites = vectors.shape
    owners = lax.axis_size("space")
    total_sites = sites * owners
    gram_scale = 1.0 / math.sqrt(48.0 * total_sites)
    loop_scale = 1.0 / math.sqrt(1.0 * total_sites)
    gamma_real, gamma_imag = pick_gammas(gamma_ids)
    spin_pick = ((dilution % 12 // 3)[:, None] == jnp.arange(4, dtype=jnp.int32)[None, :]).astype(
        jnp.float32
    )
    colour_pick = ((dilution % 3)[:, None] == jnp.arange(3, dtype=jnp.int32)[None, :]).astype(
        jnp.float32
    )
    time_class = dilution // 12
    ein = partial(jnp.einsum, precision=highest)
    lowein = partial(jnp.einsum, preferred_element_type=jnp.float32)
    first_slice = lax.axis_index("tm") * slices
    rows_real = ein("gba,ib->gia", gamma_real, spin_pick)
    rows_imag = ein("gba,ib->gia", gamma_imag, spin_pick)

    def one_slice(inputs):
        block, slice_index = inputs
        spinor = block.reshape(count, 2, 4, 3 * sites)
        real_part = spinor[:, 0]
        imag_part = spinor[:, 1]
        pair_real = lowein("iak,jbk->iajb", real_part, real_part) + lowein(
            "iak,jbk->iajb", imag_part, imag_part
        )
        pair_imag = lowein("iak,jbk->iajb", real_part, imag_part) - lowein(
            "iak,jbk->iajb", imag_part, real_part
        )
        gram_real = ein("gab,iajb->gij", gamma_real, pair_real) - ein(
            "gab,iajb->gij", gamma_imag, pair_imag
        )
        gram_imag = ein("gab,iajb->gij", gamma_real, pair_imag) + ein(
            "gab,iajb->gij", gamma_imag, pair_real
        )
        gram = jnp.concatenate([gram_real, gram_imag], axis=2).reshape(-1, 2 * count)
        gram = gram * gram_scale
        site_sums = jnp.sum(block, axis=-1, dtype=jnp.float32).reshape(count, 2, 4, 3)
        picked = ein("ipac,ic->ipa", site_sums, colour_pick)
        loop_real = ein("gia,ia->gi", rows_real, picked[:, 0]) - ein(
            "gia,ia->gi", rows_imag, picked[:, 1]
        )
        loop_imag = ein("gia,ia->gi", rows_real, picked[:, 1]) + ein(
            "gia,ia->gi", rows_imag, picked[:, 0]
        )
        live = (time_class == slice_index % TDIL).astype(jnp.float32)[None, :]
        loops = jnp.stack([loop_real * live, loop_imag * live], axis=-1).reshape(-1, 2) * loop_scale
        return (gram, loops)

    gram_terms, loop_terms = lax.map(
        one_slice, (vectors, first_slice + jnp.arange(slices, dtype=jnp.int32))
    )
    total_rows = gram_terms.shape[1]
    owned = total_rows // owners
    totals = lax.psum((gram_terms, loop_terms), "space")
    start = lax.axis_index("space") * owned
    shares = (
        lax.dynamic_slice_in_dim(totals[0], start, owned, 1),
        lax.dynamic_slice_in_dim(totals[1], start, owned, 1),
    )
    gram, loops = (
        lax.all_gather(shares[0], "tm", axis=0, tiled=True),
        lax.all_gather(shares[1], "tm", axis=0, tiled=True),
    )
    return (gram, loops)


def solution(mesh):
    placed = (P("tm", None, None, None, "space"), P(), P())
    return jax.shard_map(
        any_shards,
        mesh=mesh,
        in_specs=placed,
        out_specs=(P(None, "space", None), P(None, "space", None)),
        check_vma=False,
    )
```
